32 devices in a mesh: seq: 8 (over z, y), opt: 4 (over x, core).
Axes of the slice: x: 2, y: 2, z: 4, core: 2. Of those that a mesh axis runs over, the one named last changes fastest.
Arguments:
- layer_in: bfloat16 [4, 4096, 4096], P('opt', 'seq'), may hold values from -48 to 48, as said below
- ssm_input: bfloat16 [4, 4096, 4096], P('opt', 'seq'), may hold values from -0.119628906 to 0.119628906
- grad_out: bfloat16 [4, 4096, 4096], P('opt', 'seq'), may hold values from -0.59765625 to 0.59765625
- log_decay: float32 [4, 32, 4096], P('opt', None, 'seq'), may hold values from -1 to 0, as said below
- skip_gain: float32 [32], replicated, may hold values from 0.5 to 2
- w_bc: float32 [4096, 256], P(('seq', 'opt')), may hold values from -0.0078125 to 0.0078125
- m_code: bfloat16 [4096, 256], P(('seq', 'opt')), may hold values from -1 to 1
- m_scale: float32 [256], replicated, may hold values from 0.0001 to 0.001
- row_stat: float32 [4096], P(('seq', 'opt')), may hold values from 3e-07 to 3e-06
- col_stat: float32 [256], replicated, may hold values from 3e-07 to 3e-06
Outputs:
- grad_input: bfloat16 [4, 4096, 4096], P('opt', 'seq')
- update: float32 [4096, 256], P(('seq', 'opt'))
- code_next: bfloat16 [4096, 256], P(('seq', 'opt'))
- scale_next: float32 [256], replicated
- row_next: float32 [4096], P(('seq', 'opt'))
- col_next: float32 [256], replicated
The draws below stay inside these ranges and needn't reach their ends.
Inputs may be any that keep to these rules, and one draw needn't show every extreme that they name: `layer_in`: real-valued rows of order one. `log_decay`: negative log decays.
All inputs are finite; a program needn't handle non-finite values.
Results may differ from the reference program's by a relative error of at most 0.0095.
Values may be sent and summed in bfloat16 or wider, within the bound.
A program may use at most 256 MiB of HBM per device.

```python
import math
import jax
import jax.numpy as jnp
from jax import lax

D = 4096
N = 128
P_SIZE = 128
H = 32
BLOCK = 256
TOK_DEV = 512
TOKEN_POSITIONS = 4096
SEQUENCE_COUNT = 4


def draw_layer_in(key, part):
    lookup_keys = jax.random.split(key, 2)
    position = jnp.arange(D, dtype=jnp.float32) / (D - 1)
    feature_scale = jnp.exp(math.log(3.0) * position + math.log(10.0) * jax.random.uniform(lookup_keys[0], (D,), jnp.float32)) / 4.0
    base = jnp.clip(jax.random.normal(lookup_keys[1], (SEQUENCE_COUNT, TOKEN_POSITIONS, D), jnp.float32), -6.0, 6.0)
    return (base * feature_scale[None, None, :]).astype(jnp.bfloat16)


def draw_log_decay(key, part):
    lookup_keys = jax.random.split(key, 7)
    share = 0.5
    fast_head = jax.random.uniform(lookup_keys[0], (SEQUENCE_COUNT, H, 1), jnp.float32) < share
    fast_rate = jax.random.uniform(lookup_keys[1], (SEQUENCE_COUNT, H, 1), jnp.float32, 1.0 / 50.0, 1.0 / 30.0)
    slow_rate = jax.random.uniform(lookup_keys[2], (SEQUENCE_COUNT, H, 1), jnp.float32, 0.2, 0.6) / TOKEN_POSITIONS
    rate = jnp.where(fast_head, fast_rate, slow_rate)
    rough = jnp.exp(jax.random.uniform(lookup_keys[3], (SEQUENCE_COUNT, H, TOKEN_POSITIONS), jnp.float32, -0.7, 0.7))
    blocks = TOKEN_POSITIONS // TOK_DEV
    device_factor = jnp.exp(jax.random.uniform(lookup_keys[4], (SEQUENCE_COUNT, H, blocks, 1), jnp.float32, -0.7, 0.7))
    device_factor = jnp.broadcast_to(device_factor, (SEQUENCE_COUNT, H, blocks, TOK_DEV)).reshape(SEQUENCE_COUNT, H, TOKEN_POSITIONS)
    first_spot = jax.random.randint(lookup_keys[5], (SEQUENCE_COUNT, 1, 1, 1), 0, TOKEN_POSITIONS)
    spot_offset = jax.random.randint(jax.random.fold_in(lookup_keys[5], 1), (SEQUENCE_COUNT, 1, 1, 1), 1, TOKEN_POSITIONS)
    second_spot = (first_spot + spot_offset) % TOKEN_POSITIONS
    flurry_position = jnp.concatenate([first_spot, second_spot], axis=-1).astype(jnp.int32)
    flurry_depth = jax.random.uniform(lookup_keys[6], (SEQUENCE_COUNT, 1, 1, 2), jnp.float32, 0.22, 0.69)
    target_spots = jnp.arange(TOKEN_POSITIONS, dtype=jnp.int32)[None, None, :, None]
    match_count = jnp.sum(jnp.where(target_spots == flurry_position, flurry_depth, 0.0), axis=-1)
    return -(rate * rough * device_factor) - match_count


def steps_of(stream_key, shape, pieces, smallest, top_value):
    level, own = 1.0, jax.random.fold_in(stream_key, 6)
    for dim, parts in pieces:
        draws = jnp.exp(jax.random.uniform(jax.random.fold_in(own, dim), (parts,), jnp.float32, smallest / len(pieces), top_value / len(pieces)))
        level = level * jnp.repeat(draws, shape[dim] // parts).reshape([-1 if axis == dim else 1 for axis in range(len(shape))])
    return level


def centred(rng, dims, scale, limit, shards=(), kind=jnp.bfloat16):
    drawn = jax.random.normal(rng, dims, jnp.float32) * scale
    if len(shards) > 0:
        drawn = steps_of(rng, dims, shards, -0.22, 0.18) * drawn
    return jnp.clip(drawn, min=-limit, max=limit).astype(kind)


def setup_inputs(seed: int = 0) -> dict:
    key_of = jax.random.split(jax.random.key(seed), 11)
    layer_in = draw_layer_in(jax.random.fold_in(key_of[10], 71), 0)
    ssm_input = centred(key_of[1], (SEQUENCE_COUNT, TOKEN_POSITIONS, H * P_SIZE), 0.02, 0.119628906, ((0, 4), (1, 8)))
    grad_out = centred(key_of[2], (SEQUENCE_COUNT, TOKEN_POSITIONS, H * P_SIZE), 0.1, 0.59765625, ((0, 4), (1, 8)))
    log_decay = draw_log_decay(jax.random.fold_in(key_of[10], 71), 0)
    skip_gain = jnp.clip(jax.random.uniform(key_of[4], (H,), jnp.float32, 0.5, 2.0), 0.5, 2.0)
    w_bc = centred(key_of[5], (D, 2 * N), (D * N) ** -0.5, 0.0078125, ((0, 32),), jnp.float32)
    m_code = jnp.clip(jax.random.uniform(key_of[6], (D, 2 * N), jnp.float32, -1.0, 1.0) * steps_of(key_of[6], (D, 2 * N), ((0, 32),), -0.4, 0.0), -1.0, 1.0).astype(jnp.bfloat16)
    m_scale = jnp.clip(jnp.exp(jax.random.uniform(key_of[7], (2 * N,), jnp.float32, math.log(0.0001), math.log(0.001))), 0.0001, 0.001)
    row_stat = jnp.clip(jnp.exp(math.log(3.000000106112566e-06) - 2.3025851 * jax.random.uniform(key_of[8], (D,), jnp.float32) ** steps_of(key_of[8], (D,), ((0, 32),), -0.2, 0.2)), 3.000000106112566e-07, 3.000000106112566e-06)
    col_stat = jnp.clip(jnp.exp(jax.random.uniform(key_of[9], (2 * N,), jnp.float32, math.log(3.000000106112566e-07), math.log(3.000000106112566e-06))), 3.000000106112566e-07, 3.000000106112566e-06)
    return {"layer_in": layer_in, "ssm_input": ssm_input, "grad_out": grad_out, "log_decay": log_decay, "skip_gain": skip_gain, "w_bc": w_bc, "m_code": m_code, "m_scale": m_scale, "row_stat": row_stat, "col_stat": col_stat}


beta_one = 0.9
beta_two = 0.95
weight_decay = 0.1
clip_norm = 1.0
tiny_square = 1e-30
adam_floor = 1e-08
peak_floor = 1e-06
norm_floor = 1e-06
highest = lax.Precision.HIGHEST

def lower_decays(running):
    length = running.shape[1]
    row_pos = lax.broadcasted_iota(jnp.int32, (length, length), 0)
    col_pos = lax.broadcasted_iota(jnp.int32, (length, length), 1)
    spread = running[:, :, None] - running[:, None, :]
    return jnp.exp(jnp.where((row_pos >= col_pos)[None], spread, -jnp.inf))

def state_adds(feat_blk, cot_blk, b_rows, c_rows, running):
    closing = running[:, -1]
    shrink = jnp.exp(closing[:, None] - running)
    grow = jnp.exp(running)
    forward_add = jnp.einsum('htn,thp->hnp', shrink[:, :, None] * b_rows[None], feat_blk, precision=highest)
    backward_add = jnp.einsum('htn,thp->hnp', grow[:, :, None] * c_rows[None], cot_blk, precision=highest)
    return (forward_add, backward_add)

def block_terms(feat_blk, cot_blk, b_rows, c_rows, running, state_in, grad_in, skip_gain):
    closing = running[:, -1]
    decays = lower_decays(running)
    grow = jnp.exp(running)
    shrink = jnp.exp(closing[:, None] - running)
    intersection = jnp.einsum('thp,shp->hts', feat_blk, cot_blk, precision=highest)
    affinity = jnp.dot(b_rows, c_rows.T, precision=highest)
    mixing = lax.optimization_barrier(jnp.sum(decays * jnp.transpose(intersection, (0, 2, 1)), axis=0))
    left_in = jnp.einsum('hnp,thp->htn', state_in, cot_blk, precision=highest)
    grad_cmat = jnp.dot(mixing, b_rows, precision=highest) + lax.optimization_barrier(jnp.sum(grow[:, :, None] * left_in, axis=0))
    right_in = jnp.einsum('hnp,thp->htn', grad_in, feat_blk, precision=highest)
    grad_bmat = jnp.dot(mixing.T, c_rows, precision=highest) + lax.optimization_barrier(jnp.sum(shrink[:, :, None] * right_in, axis=0))
    weighted = jnp.transpose(decays, (0, 2, 1)) * affinity[None]
    inner = jnp.einsum('hts,shp->thp', weighted, cot_blk, precision=highest)
    outer = jnp.einsum('tn,hnp->thp', b_rows, grad_in, precision=highest) * shrink.T[:, :, None]
    grad_feat = inner + outer + skip_gain[None, :, None] * cot_blk
    return (grad_feat, jnp.concatenate([grad_bmat, grad_cmat], axis=1))

def one_sequence(layer_rows, feat_rows, cot_rows, log_rows, w_half, skip_gain):
    proj = jnp.dot(layer_rows, w_half, preferred_element_type=jnp.float32).astype(jnp.bfloat16)
    count = TOKEN_POSITIONS // BLOCK
    b_all = proj[:, :N].astype(jnp.float32).reshape(count, BLOCK, N)
    c_all = proj[:, N:].astype(jnp.float32).reshape(count, BLOCK, N)
    feats = feat_rows.astype(jnp.float32).reshape(count, BLOCK, H, P_SIZE)
    cots = cot_rows.astype(jnp.float32).reshape(count, BLOCK, H, P_SIZE)
    logs = jnp.transpose(log_rows.reshape(H, count, BLOCK), (1, 0, 2))

    def forward(state, items):
        feat_blk, cot_blk, b_rows, c_rows, log_blk = items
        running = jnp.cumsum(log_blk, axis=1)
        forward_add, unused = state_adds(feat_blk, cot_blk, b_rows, c_rows, running)
        return (jnp.exp(running[:, -1])[:, None, None] * state + forward_add, state)
    start = jnp.zeros((H, N, P_SIZE), jnp.float32)
    unused_last, states_in = lax.scan(forward, start, (feats, cots, b_all, c_all, logs))

    def backward(grad_in, items):
        feat_blk, cot_blk, b_rows, c_rows, log_blk, state_in = items
        running = jnp.cumsum(log_blk, axis=1)
        grad_feat, grad_bc = block_terms(feat_blk, cot_blk, b_rows, c_rows, running, state_in, grad_in, skip_gain)
        unused, backward_add = state_adds(feat_blk, cot_blk, b_rows, c_rows, running)
        return (jnp.exp(running[:, -1])[:, None, None] * grad_in + backward_add, (grad_feat, grad_bc))
    unused_first, outputs = lax.scan(backward, start, (feats, cots, b_all, c_all, logs, states_in), reverse=True)
    grad_feats, grad_bcs = outputs
    grad_bc = grad_bcs.reshape(TOKEN_POSITIONS, 2 * N).astype(jnp.bfloat16)
    weight_grad = jnp.dot(layer_rows.T, grad_bc, preferred_element_type=jnp.float32)
    return (grad_feats.reshape(TOKEN_POSITIONS, H * P_SIZE).astype(jnp.bfloat16), weight_grad)

def reference(layer_in, ssm_input, grad_out, log_decay, skip_gain, w_bc, m_code, m_scale, row_stat, col_stat):
    w_half = w_bc.astype(jnp.bfloat16)
    results = []
    grad_sum = jnp.zeros((D, 2 * N), jnp.float32)
    for seq_id in range(SEQUENCE_COUNT):
        grad_feat, weight_grad = one_sequence(layer_in[seq_id], ssm_input[seq_id], grad_out[seq_id], log_decay[seq_id], w_half, skip_gain)
        results.append(grad_feat)
        grad_sum = grad_sum + weight_grad
    grad_input = jnp.stack(results)
    norm_sq = jnp.sum(grad_sum * grad_sum) + norm_floor
    factor = jnp.minimum(1.0, clip_norm / jnp.sqrt(norm_sq))
    scaled = grad_sum * factor
    squares = scaled * scaled
    moment = beta_one * m_code.astype(jnp.float32) * m_scale[None, :] + (1.0 - beta_one) * scaled
    row_next = beta_two * row_stat + (1.0 - beta_two) * (lax.optimization_barrier(jnp.mean(squares, axis=1)) + tiny_square)
    col_next = beta_two * col_stat + (1.0 - beta_two) * (lax.optimization_barrier(jnp.mean(squares, axis=0)) + tiny_square)
    second = row_next[:, None] * col_next[None, :] / jnp.mean(row_next)
    update = moment / (jnp.sqrt(second) + adam_floor) + weight_decay * w_bc
    scale_next = lax.optimization_barrier(jnp.max(jnp.abs(moment), axis=0)) + peak_floor
    code_next = (moment / scale_next[None, :]).astype(jnp.bfloat16)
    return (grad_input, update, code_next, scale_next, row_next, col_next)
```

```python
import functools

import jax
import jax.numpy as jnp
from jax import lax
from jax.experimental import pallas as pl
from jax.experimental.pallas import tpu as pltpu
from jax.sharding import PartitionSpec as P

BLOCK = 256
LANES = 128

beta_one = 0.9
beta_two = 0.95
weight_decay = 0.1
clip_norm = 1.0
tiny_square = 1e-30
adam_floor = 1e-08
peak_floor = 1e-06
norm_floor = 1e-06
highest = lax.Precision.HIGHEST
MESH = pl.DeviceIdType.MESH
VMEM_LIMIT = 60 * 1024 * 1024
f32 = jnp.float32
bf16 = jnp.bfloat16


def dot_nn(a, b):
    return lax.dot_general(a, b, (((1,), (0,)), ((), ())), preferred_element_type=f32)


def dot_nt(a, b):
    return lax.dot_general(a, b, (((1,), (1,)), ((), ())), preferred_element_type=f32)


def dot_tn(a, b):
    return lax.dot_general(a, b, (((0,), (0,)), ((), ())), preferred_element_type=f32)


def as_column(row):
    return jnp.transpose(jnp.broadcast_to(row, (LANES, row.shape[1])))


def widened(column, length):
    return jnp.concatenate([column] * (length // LANES), axis=1)


def mixing_kernel(count, x_ref, dy_ref, run_ref, mix_ref):
    @pl.when(pl.program_id(0) == 0)
    def _():
        mix_ref[...] = jnp.zeros_like(mix_ref)

    row_pos = lax.broadcasted_iota(jnp.int32, (BLOCK, BLOCK), 0)
    col_pos = lax.broadcasted_iota(jnp.int32, (BLOCK, BLOCK), 1)
    for b in range(count):
        rows = slice(b * BLOCK, (b + 1) * BLOCK)
        row = run_ref[0, b : b + 1, :]
        spread = widened(as_column(row), BLOCK) - row
        decays = jnp.exp(jnp.where(row_pos >= col_pos, spread, -jnp.inf))
        mix_ref[b] += decays * dot_nt(dy_ref[rows, :], x_ref[rows, :])


def local_kernel(count, x_ref, dy_ref, b_ref, c_ref, run_ref, send_ref, starts_ref, outs_ref):
    adds = []
    for b in range(count):
        rows = slice(b * BLOCK, (b + 1) * BLOCK)
        row = run_ref[0, b : b + 1, :]
        column = as_column(row)
        closing = row[:, BLOCK - 1 : BLOCK]
        b_scaled = (b_ref[rows, :].astype(f32) * jnp.exp(closing - column)).astype(bf16)
        c_scaled = (c_ref[rows, :].astype(f32) * jnp.exp(column)).astype(bf16)
        adds.append(
            (jnp.exp(closing), dot_tn(b_scaled, x_ref[rows, :]), dot_tn(c_scaled, dy_ref[rows, :]))
        )
    state = None
    for b in range(count):
        starts_ref[0, b] = (jnp.zeros_like(adds[b][1]) if state is None else state).astype(bf16)
        state = adds[b][1] if state is None else adds[b][0] * state + adds[b][1]
    send_ref[0, 0, 0] = state.astype(bf16)
    carried = None
    for b in reversed(range(count)):
        outs_ref[0, b] = (jnp.zeros_like(adds[b][2]) if carried is None else carried).astype(bf16)
        carried = adds[b][2] if carried is None else adds[b][0] * carried + adds[b][2]
    send_ref[0, 1, 0] = carried.astype(bf16)


def grads_kernel(
    count, skip_ref, x_ref, dy_ref, b_ref, c_ref, run_ref, starts_ref, outs_ref, far_ref, mix_ref,
    gx_ref, gbc_ref, affinity, acc_b, acc_c,
):
    h = pl.program_id(0)
    state_dim = b_ref.shape[1]

    @pl.when(h == 0)
    def _():
        acc_b[...] = jnp.zeros_like(acc_b)
        acc_c[...] = jnp.zeros_like(acc_c)
        for b in range(count):
            rows = slice(b * BLOCK, (b + 1) * BLOCK)
            affinity[b] = dot_nt(b_ref[rows, :], c_ref[rows, :])

    row_pos = lax.broadcasted_iota(jnp.int32, (BLOCK, BLOCK), 0)
    col_pos = lax.broadcasted_iota(jnp.int32, (BLOCK, BLOCK), 1)
    closings = [run_ref[0, b : b + 1, BLOCK - 1 : BLOCK] for b in range(count)]
    for b in range(count):
        rows = slice(b * BLOCK, (b + 1) * BLOCK)
        row = run_ref[0, b : b + 1, :]
        column = as_column(row)
        before = sum(closings[:b], jnp.zeros((1, 1), f32))
        after = sum(closings[b + 1 :], jnp.zeros((1, 1), f32))
        far_state = far_ref[0, 0, 0].astype(f32)
        far_grad = far_ref[0, 1, 0].astype(f32)
        state_in = (starts_ref[0, b].astype(f32) + jnp.exp(before) * far_state).astype(bf16)
        grad_in = (outs_ref[0, b].astype(f32) + jnp.exp(after) * far_grad).astype(bf16)
        grow = jnp.exp(column)
        shrink = jnp.exp(closings[b] - column)
        x_blk = x_ref[rows, :]
        dy_blk = dy_ref[rows, :]
        spread = row - widened(column, BLOCK)
        decays = jnp.exp(jnp.where(col_pos >= row_pos, spread, -jnp.inf))
        weighted = (decays * affinity[b]).astype(bf16)
        inner = dot_nn(weighted, dy_blk)
        outer = dot_nn(b_ref[rows, :], grad_in) * shrink
        gx_ref[rows, :] = (inner + outer + skip_ref[h] * dy_blk.astype(f32)).astype(bf16)
        acc_c[rows, :] += grow * dot_nt(dy_blk, state_in)
        acc_b[rows, :] += shrink * dot_nt(x_blk, grad_in)

    @pl.when(h == pl.num_programs(0) - 1)
    def _():
        for b in range(count):
            rows = slice(b * BLOCK, (b + 1) * BLOCK)
            mixing = mix_ref[b].astype(bf16)
            gbc_ref[rows, :state_dim] = (acc_b[rows, :] + dot_tn(mixing, c_ref[rows, :])).astype(bf16)
            gbc_ref[rows, state_dim:] = (acc_c[rows, :] + dot_nn(mixing, b_ref[rows, :])).astype(bf16)


def swap_all(n, me, src_of, dst_of, device_of, send_sem, recv_sem):
    def copy_to(distance):
        other = lax.rem(me + distance, n)
        return pltpu.make_async_remote_copy(
            src_ref=src_of(other), dst_ref=dst_of(me), send_sem=send_sem.at[other],
            recv_sem=recv_sem.at[me], device_id=device_of(other), device_id_type=MESH,
        )

    def copy_from(distance):
        other = lax.rem(me + distance, n)
        return pltpu.make_async_remote_copy(
            src_ref=src_of(other), dst_ref=dst_of(other), send_sem=send_sem.at[other],
            recv_sem=recv_sem.at[other], device_id=device_of(other), device_id_type=MESH,
        )

    def start(distance, carry):
        copy_to(distance).start()
        return carry

    def finish(distance, carry):
        copy = copy_from(distance)
        copy.wait_send()
        copy.wait_recv()
        return carry

    lax.fori_loop(1, n, start, 0)
    return lambda: lax.fori_loop(1, n, finish, 0)


def greet(n, me, device_of):
    barrier = pltpu.get_barrier_semaphore()

    def signal(distance, carry):
        other = lax.rem(me + distance, n)
        pl.semaphore_signal(barrier, inc=1, device_id=device_of(other), device_id_type=MESH)
        return carry

    lax.fori_loop(1, n, signal, 0)
    pl.semaphore_wait(barrier, n - 1)


def carry_kernel(
    n, send_ref, decay_ref, out_ref, got, got_decay, prefix, landed, run,
    send_a, recv_a, send_d, recv_d, send_b, recv_b,
):
    me = lax.axis_index("seq")
    opt = lax.axis_index("opt")

    def device_of(s):
        return (s, opt)

    greet(n, me, device_of)
    end_d = swap_all(
        n, me, lambda s: decay_ref.at[s], lambda s: got_decay.at[s], device_of, send_d, recv_d
    )
    end_a = swap_all(n, me, lambda s: send_ref.at[s], lambda s: got.at[s], device_of, send_a, recv_a)
    end_d()
    end_a()
    got[me] = send_ref[me]
    got_decay[me] = decay_ref[me]

    run[...] = jnp.zeros_like(run)

    def forward(s, carry):
        state = run[0]
        prefix[s, 0] = state.astype(bf16)
        run[0] = got_decay[s] * state + got[s, 0].astype(f32)
        return carry

    def backward(lap, carry):
        s = n - 1 - lap
        state = run[1]
        prefix[s, 1] = state.astype(bf16)
        run[1] = got_decay[s] * state + got[s, 1].astype(f32)
        return carry

    lax.fori_loop(0, n, forward, 0)
    lax.fori_loop(0, n, backward, 0)
    swap_all(n, me, lambda s: prefix.at[s], lambda s: landed.at[s], device_of, send_b, recv_b)()
    landed[me] = prefix[me]
    out_ref[...] = landed[...]


def step_kernel(
    n_seq, n_opt, part_ref, w_ref, code_ref, scale_ref, row_ref, col_ref,
    update_ref, code_out, scale_out, row_out, col_out,
    got_a, mid, got_b, stats, all_stats, peak, all_peaks,
    send_a, recv_a, send_b, recv_b, send_c, recv_c, send_d, recv_d,
):
    seq = lax.axis_index("seq")
    opt = lax.axis_index("opt")
    n = n_seq * n_opt
    me = seq * n_opt + opt

    def any_device(i):
        return (i // n_opt, lax.rem(i, n_opt))

    greet(n, me, any_device)
    swap_all(
        n_opt, opt, lambda o: part_ref.at[o], lambda o: got_a.at[o],
        lambda o: (seq, o), send_a, recv_a,
    )()
    got_a[opt] = part_ref[opt]

    def fold(s, carry):
        total = got_a[0, s].astype(f32)
        for o in range(1, n_opt):
            total += got_a[o, s].astype(f32)
        mid[s] = total.astype(bf16)
        return carry

    lax.fori_loop(0, n_seq, fold, 0)
    swap_all(
        n_seq, seq, lambda s: mid.at[s], lambda s: got_b.at[s],
        lambda s: (s, opt), send_b, recv_b,
    )()
    got_b[seq] = mid[seq]
    grad = got_b[0].astype(f32)
    for s in range(1, n_seq):
        grad += got_b[s].astype(f32)

    rows, cols = grad.shape
    width = n * rows
    squares_raw = grad * grad
    stats[:, :cols] = jnp.sum(squares_raw, axis=0, keepdims=True)
    row_stat = row_ref[...]
    stats[:, cols:] = jnp.broadcast_to(jnp.sum(row_stat, axis=0, keepdims=True), (1, LANES))
    swap_all(
        n, me, lambda i: stats, lambda i: all_stats.at[i], any_device, send_c, recv_c
    )()
    all_stats[me] = stats[...]
    sums = all_stats[0]
    for i in range(1, n):
        sums += all_stats[i]
    col_raw = sums[:, :cols]
    old_total = sums[:, cols : cols + 1]
    raw_total = jnp.sum(col_raw, axis=1, keepdims=True)
    factor = jnp.minimum(1.0, clip_norm / jnp.sqrt(raw_total + norm_floor))
    scaled = grad * factor
    moment = beta_one * code_ref[...].astype(f32) * scale_ref[...] + (1.0 - beta_one) * scaled
    peak[...] = jnp.max(jnp.abs(moment), axis=0, keepdims=True)
    end_peaks = swap_all(
        n, me, lambda i: peak, lambda i: all_peaks.at[i], any_device, send_d, recv_d
    )
    col_next = beta_two * col_ref[...] + (1.0 - beta_two) * (
        factor * factor * col_raw / width + tiny_square
    )
    row_next = beta_two * row_stat + (1.0 - beta_two) * (
        jnp.sum(scaled * scaled, axis=1, keepdims=True) / cols + tiny_square
    )
    row_mean = (
        beta_two * old_total
        + (1.0 - beta_two) * (factor * factor * raw_total / cols + width * tiny_square)
    ) / width
    second = row_next * col_next / row_mean
    update_ref[...] = moment / (jnp.sqrt(second) + adam_floor) + weight_decay * w_ref[...]
    row_out[...] = row_next
    col_out[...] = col_next
    end_peaks()
    all_peaks[me] = peak[...]
    scale_next = all_peaks[0]
    for i in range(1, n):
        scale_next = jnp.maximum(scale_next, all_peaks[i])
    scale_next = scale_next + peak_floor
    scale_out[...] = scale_next
    code_out[...] = (moment / scale_next).astype(bf16)


def params(**more):
    return pltpu.CompilerParams(vmem_limit_bytes=VMEM_LIMIT, **more)


def whole():
    return pl.BlockSpec(memory_space=pltpu.VMEM)


def dma(*counts):
    return [pltpu.SemaphoreType.DMA((count,)) for count in counts for _ in range(2)]


def per_device(
    n_seq, n_opt, layer_in, ssm_input, grad_out, log_decay, skip_gain, w_bc, m_code, m_scale,
    row_stat, col_stat,
):
    layer_rows = layer_in[0]
    x = ssm_input[0]
    dy = grad_out[0]
    length, width = layer_rows.shape
    heads = skip_gain.shape[0]
    head_dim = x.shape[1] // heads
    state_dim = w_bc.shape[1] // 2
    count = length // BLOCK
    group = heads // n_seq
    own_rows = w_bc.shape[0]

    w_all = lax.all_gather(w_bc.astype(bf16), ("seq", "opt"), axis=0, tiled=True)

    ones = (
        lax.broadcasted_iota(jnp.int32, (BLOCK, BLOCK), 0)
        <= lax.broadcasted_iota(jnp.int32, (BLOCK, BLOCK), 1)
    ).astype(f32)
    running = jnp.dot(
        log_decay[0].reshape(heads * count, BLOCK), ones, precision=highest
    ).reshape(heads, count, BLOCK)
    decay = jnp.exp(jnp.sum(running[:, :, BLOCK - 1], axis=1))
    decay = jnp.broadcast_to(decay[:, None], (heads, LANES)).reshape(n_seq, group, 1, LANES)

    tokens = pl.BlockSpec((length, head_dim), lambda h: (0, h))
    run_spec = pl.BlockSpec((1, count, BLOCK), lambda h: (h, 0, 0))
    mix_spec = pl.BlockSpec((count, BLOCK, BLOCK), lambda h: (0, 0, 0))
    state_spec = pl.BlockSpec((1, count, state_dim, head_dim), lambda h: (h, 0, 0, 0))
    far_spec = pl.BlockSpec(
        (1, 2, 1, state_dim, head_dim), lambda h: (h // group, 0, h % group, 0, 0)
    )
    b_spec = pl.BlockSpec((length, state_dim), lambda h: (0, 0))
    c_spec = pl.BlockSpec((length, state_dim), lambda h: (0, 1))
    far_shape = (n_seq, 2, group, state_dim, head_dim)
    square = heads * length * BLOCK

    mixing = pl.pallas_call(
        functools.partial(mixing_kernel, count),
        grid=(heads,),
        in_specs=[tokens, tokens, run_spec],
        out_specs=mix_spec,
        out_shape=jax.ShapeDtypeStruct((count, BLOCK, BLOCK), f32),
        compiler_params=params(),
        cost_estimate=pl.CostEstimate(
            flops=2 * square * head_dim * 10, bytes_accessed=4 * length * width, transcendentals=square
        ),
        name="mixing",
    )(x, dy, running)

    proj = jnp.dot(layer_rows, w_all, preferred_element_type=f32).astype(bf16)

    sent, starts, outs = pl.pallas_call(
        functools.partial(local_kernel, count),
        grid=(heads,),
        in_specs=[tokens, tokens, b_spec, c_spec, run_spec],
        out_specs=[far_spec, state_spec, state_spec],
        out_shape=[
            jax.ShapeDtypeStruct(far_shape, bf16),
            jax.ShapeDtypeStruct((heads, count, state_dim, head_dim), bf16),
            jax.ShapeDtypeStruct((heads, count, state_dim, head_dim), bf16),
        ],
        compiler_params=params(),
        name="local_states",
    )(x, dy, proj, proj, running)

    far = pl.pallas_call(
        functools.partial(carry_kernel, n_seq),
        in_specs=[whole(), whole()],
        out_specs=whole(),
        out_shape=jax.ShapeDtypeStruct(far_shape, bf16),
        scratch_shapes=[
            pltpu.VMEM(far_shape, bf16),
            pltpu.VMEM((n_seq, group, 1, LANES), f32),
            pltpu.VMEM(far_shape, bf16),
            pltpu.VMEM(far_shape, bf16),
            pltpu.VMEM(far_shape[1:], f32),
        ]
        + dma(n_seq, n_seq, n_seq),
        compiler_params=params(collective_id=0, has_side_effects=True),
        name="carry_states",
    )(sent, decay)

    grad_input, grad_bc = pl.pallas_call(
        functools.partial(grads_kernel, count),
        grid=(heads,),
        in_specs=[
            pl.BlockSpec(memory_space=pltpu.SMEM), tokens, tokens, b_spec, c_spec, run_spec,
            state_spec, state_spec, far_spec, mix_spec,
        ],
        out_specs=[tokens, pl.BlockSpec((length, 2 * state_dim), lambda h: (0, 0))],
        out_shape=[
            jax.ShapeDtypeStruct(x.shape, bf16),
            jax.ShapeDtypeStruct((length, 2 * state_dim), bf16),
        ],
        scratch_shapes=[
            pltpu.VMEM((count, BLOCK, BLOCK), f32),
            pltpu.VMEM((length, state_dim), f32),
            pltpu.VMEM((length, state_dim), f32),
        ],
        compiler_params=params(),
        name="grads",
    )(skip_gain, x, dy, proj, proj, running, starts, outs, far, mixing)

    cols = 2 * state_dim
    part = lax.dot_general(
        layer_rows, grad_bc, (((0,), (0,)), ((), ())), preferred_element_type=f32
    ).astype(bf16)
    part = jnp.transpose(part.reshape(n_seq, n_opt, own_rows, cols), (1, 0, 2, 3))

    n = n_seq * n_opt
    update, code_next, scale_next, row_next, col_next = pl.pallas_call(
        functools.partial(step_kernel, n_seq, n_opt),
        in_specs=[whole()] * 6,
        out_specs=[whole()] * 5,
        out_shape=[
            jax.ShapeDtypeStruct((own_rows, cols), f32),
            jax.ShapeDtypeStruct((own_rows, cols), bf16),
            jax.ShapeDtypeStruct((1, cols), f32),
            jax.ShapeDtypeStruct((own_rows, 1), f32),
            jax.ShapeDtypeStruct((1, cols), f32),
        ],
        scratch_shapes=[
            pltpu.VMEM((n_opt, n_seq, own_rows, cols), bf16),
            pltpu.VMEM((n_seq, own_rows, cols), bf16),
            pltpu.VMEM((n_seq, own_rows, cols), bf16),
            pltpu.VMEM((1, cols + LANES), f32),
            pltpu.VMEM((n, 1, cols + LANES), f32),
            pltpu.VMEM((1, cols), f32),
            pltpu.VMEM((n, 1, cols), f32),
        ]
        + dma(n_opt, n_seq, n, n),
        compiler_params=params(collective_id=1, has_side_effects=True),
        name="sum_and_step",
    )(part, w_bc, m_code, m_scale[None, :], row_stat[:, None], col_stat[None, :])
    return (grad_input[None], update, code_next, scale_next[0], row_next[:, 0], col_next[0])


def solution(mesh):
    return jax.shard_map(
        functools.partial(per_device, mesh.shape["seq"], mesh.shape["opt"]),
        mesh=mesh,
        in_specs=(
            P("opt", "seq", None),
            P("opt", "seq", None),
            P("opt", "seq", None),
            P("opt", None, "seq"),
            P(),
            P(("seq", "opt"), None),
            P(("seq", "opt"), None),
            P(),
            P(("seq", "opt")),
            P(),
        ),
        out_specs=(
            P("opt", "seq", None),
            P(("seq", "opt"), None),
            P(("seq", "opt"), None),
            P(),
            P(("seq", "opt")),
            P(),
        ),
        check_vma=False,
    )
```

```python
import functools

import jax
import jax.numpy as jnp
from jax import lax
from jax.experimental import pallas as pl
from jax.experimental.pallas import tpu as pltpu
from jax.sharding import PartitionSpec as P

BLOCK = 256
LANES = 128

beta_one = 0.9
beta_two = 0.95
weight_decay = 0.1
clip_norm = 1.0
tiny_square = 1e-30
adam_floor = 1e-08
peak_floor = 1e-06
norm_floor = 1e-06
highest = lax.Precision.HIGHEST
MESH = pl.DeviceIdType.MESH
VMEM_LIMIT = 60 * 1024 * 1024
f32 = jnp.float32
bf16 = jnp.bfloat16


def dot_nn(a, b):
    return lax.dot_general(a, b, (((1,), (0,)), ((), ())), preferred_element_type=f32)


def dot_nt(a, b):
    return lax.dot_general(a, b, (((1,), (1,)), ((), ())), preferred_element_type=f32)


def dot_tn(a, b):
    return lax.dot_general(a, b, (((0,), (0,)), ((), ())), preferred_element_type=f32)


def as_column(row):
    return jnp.transpose(jnp.broadcast_to(row, (LANES, row.shape[1])))


def widened(column, length):
    return jnp.concatenate([column] * (length // LANES), axis=1)


def mixing_kernel(
    count, n_seq, n_opt, w_ref, x_ref, dy_ref, run_ref, mix_ref, w_out,
    got, send_a, recv_a, send_b, recv_b,
):
    seq = lax.axis_index("seq")
    opt = lax.axis_index("opt")
    h = pl.program_id(0)
    last = pl.num_programs(0) - 1

    def over_seq():
        return swap_all(
            n_seq, seq, lambda s: w_ref, lambda s: got.at[opt, s],
            lambda s: (s, opt), send_a, recv_a,
        )

    def over_opt():
        return swap_all(
            n_opt, opt, lambda o: got.at[opt], lambda o: got.at[o],
            lambda o: (seq, o), send_b, recv_b,
        )

    @pl.when(h == 0)
    def _():
        greet(n_seq * n_opt, seq * n_opt + opt, lambda i: (i // n_opt, lax.rem(i, n_opt)))
        over_seq()[0]()
        got[opt, seq] = w_ref[...]
        mix_ref[...] = jnp.zeros_like(mix_ref)

    @pl.when(h == last // 2)
    def _():
        over_seq()[1]()
        over_opt()[0]()

    row_pos = lax.broadcasted_iota(jnp.int32, (BLOCK, BLOCK), 0)
    col_pos = lax.broadcasted_iota(jnp.int32, (BLOCK, BLOCK), 1)
    for b in range(count):
        rows = slice(b * BLOCK, (b + 1) * BLOCK)
        row = run_ref[0, b : b + 1, :]
        spread = widened(as_column(row), BLOCK) - row
        decays = jnp.exp(jnp.where(row_pos >= col_pos, spread, -jnp.inf))
        mix_ref[b] += decays * dot_nt(dy_ref[rows, :], x_ref[rows, :])

    @pl.when(h == last)
    def _():
        over_opt()[1]()

        def place(s, carry):
            for o in range(n_opt):
                w_out[s, o] = got[o, s]
            return carry

        lax.fori_loop(0, n_seq, place, 0)


def local_kernel(
    count, x_ref, dy_ref, b_ref, c_ref, run_ref, send_ref, starts_ref, outs_ref, b_turned, c_turned
):
    @pl.when(pl.program_id(0) == 0)
    def _():
        b_turned[...] = jnp.transpose(b_ref[...].astype(f32))
        c_turned[...] = jnp.transpose(c_ref[...].astype(f32))

    adds = []
    for b in range(count):
        rows = slice(b * BLOCK, (b + 1) * BLOCK)
        row = run_ref[0, b : b + 1, :]
        closing = row[:, BLOCK - 1 : BLOCK]
        b_scaled = (b_turned[:, rows] * jnp.exp(closing - row)).astype(bf16)
        c_scaled = (c_turned[:, rows] * jnp.exp(row)).astype(bf16)
        adds.append(
            (jnp.exp(closing), dot_nn(b_scaled, x_ref[rows, :]), dot_nn(c_scaled, dy_ref[rows, :]))
        )
    state = None
    for b in range(count):
        starts_ref[0, b] = (jnp.zeros_like(adds[b][1]) if state is None else state).astype(bf16)
        state = adds[b][1] if state is None else adds[b][0] * state + adds[b][1]
    send_ref[0, 0, 0] = state.astype(bf16)
    carried = None
    for b in reversed(range(count)):
        outs_ref[0, b] = (jnp.zeros_like(adds[b][2]) if carried is None else carried).astype(bf16)
        carried = adds[b][2] if carried is None else adds[b][0] * carried + adds[b][2]
    send_ref[0, 1, 0] = carried.astype(bf16)


def grads_kernel(
    count, skip_ref, x_ref, dy_ref, b_ref, c_ref, run_ref, starts_ref, outs_ref, far_ref, mix_ref,
    gx_ref, gbc_ref, affinity, acc_b, acc_c,
):
    h = pl.program_id(0)
    state_dim = b_ref.shape[1]

    @pl.when(h == 0)
    def _():
        acc_b[...] = jnp.zeros_like(acc_b)
        acc_c[...] = jnp.zeros_like(acc_c)
        for b in range(count):
            rows = slice(b * BLOCK, (b + 1) * BLOCK)
            affinity[b] = dot_nt(b_ref[rows, :], c_ref[rows, :])

    row_pos = lax.broadcasted_iota(jnp.int32, (BLOCK, BLOCK), 0)
    col_pos = lax.broadcasted_iota(jnp.int32, (BLOCK, BLOCK), 1)
    closings = [run_ref[0, b : b + 1, BLOCK - 1 : BLOCK] for b in range(count)]
    for b in range(count):
        rows = slice(b * BLOCK, (b + 1) * BLOCK)
        row = run_ref[0, b : b + 1, :]
        column = as_column(row)
        before = sum(closings[:b], jnp.zeros((1, 1), f32))
        after = sum(closings[b + 1 :], jnp.zeros((1, 1), f32))
        far_state = far_ref[0, 0, 0].astype(f32)
        far_grad = far_ref[0, 1, 0].astype(f32)
        state_in = (starts_ref[0, b].astype(f32) + jnp.exp(before) * far_state).astype(bf16)
        grad_in = (outs_ref[0, b].astype(f32) + jnp.exp(after) * far_grad).astype(bf16)
        grow = jnp.exp(column)
        shrink = jnp.exp(closings[b] - column)
        x_blk = x_ref[rows, :]
        dy_blk = dy_ref[rows, :]
        spread = row - widened(column, BLOCK)
        decays = jnp.exp(jnp.where(col_pos >= row_pos, spread, -jnp.inf))
        weighted = (decays * affinity[b]).astype(bf16)
        inner = dot_nn(weighted, dy_blk)
        outer = dot_nn(b_ref[rows, :], grad_in) * shrink
        gx_ref[rows, :] = (inner + outer + skip_ref[h] * dy_blk.astype(f32)).astype(bf16)
        acc_c[rows, :] += grow * dot_nt(dy_blk, state_in)
        acc_b[rows, :] += shrink * dot_nt(x_blk, grad_in)

    @pl.when(h == pl.num_programs(0) - 1)
    def _():
        for b in range(count):
            rows = slice(b * BLOCK, (b + 1) * BLOCK)
            mixing = mix_ref[b].astype(bf16)
            gbc_ref[rows, :state_dim] = (acc_b[rows, :] + dot_tn(mixing, c_ref[rows, :])).astype(bf16)
            gbc_ref[rows, state_dim:] = (acc_c[rows, :] + dot_nn(mixing, b_ref[rows, :])).astype(bf16)


def swap_all(n, me, src_of, dst_of, device_of, send_sem, recv_sem):
    def copy_to(distance):
        other = lax.rem(me + distance, n)
        return pltpu.make_async_remote_copy(
            src_ref=src_of(other), dst_ref=dst_of(me), send_sem=send_sem.at[other],
            recv_sem=recv_sem.at[me], device_id=device_of(other), device_id_type=MESH,
        )

    def copy_from(distance):
        other = lax.rem(me + distance, n)
        return pltpu.make_async_remote_copy(
            src_ref=src_of(other), dst_ref=dst_of(other), send_sem=send_sem.at[other],
            recv_sem=recv_sem.at[other], device_id=device_of(other), device_id_type=MESH,
        )

    def start(distance, carry):
        copy_to(distance).start()
        return carry

    def finish(distance, carry):
        copy = copy_from(distance)
        copy.wait_send()
        copy.wait_recv()
        return carry

    return lambda: lax.fori_loop(1, n, start, 0), lambda: lax.fori_loop(1, n, finish, 0)


def begin_swap(*args):
    start, finish = swap_all(*args)
    start()
    return finish


def greet(n, me, device_of):
    barrier = pltpu.get_barrier_semaphore()

    def signal(distance, carry):
        other = lax.rem(me + distance, n)
        pl.semaphore_signal(barrier, inc=1, device_id=device_of(other), device_id_type=MESH)
        return carry

    lax.fori_loop(1, n, signal, 0)
    pl.semaphore_wait(barrier, n - 1)


def carry_kernel(
    n, send_ref, decay_ref, out_ref, got, got_decay, prefix, landed, run,
    send_a, recv_a, send_d, recv_d, send_b, recv_b,
):
    me = lax.axis_index("seq")
    opt = lax.axis_index("opt")

    def device_of(s):
        return (s, opt)

    greet(n, me, device_of)
    end_d = begin_swap(
        n, me, lambda s: decay_ref.at[s], lambda s: got_decay.at[s], device_of, send_d, recv_d
    )
    end_a = begin_swap(n, me, lambda s: send_ref.at[s], lambda s: got.at[s], device_of, send_a, recv_a)
    end_d()
    end_a()
    got[me] = send_ref[me]
    got_decay[me] = decay_ref[me]

    run[...] = jnp.zeros_like(run)

    def forward(s, carry):
        state = run[0]
        prefix[s, 0] = state.astype(bf16)
        run[0] = got_decay[s] * state + got[s, 0].astype(f32)
        return carry

    def backward(lap, carry):
        s = n - 1 - lap
        state = run[1]
        prefix[s, 1] = state.astype(bf16)
        run[1] = got_decay[s] * state + got[s, 1].astype(f32)
        return carry

    lax.fori_loop(0, n, forward, 0)
    lax.fori_loop(0, n, backward, 0)
    begin_swap(n, me, lambda s: prefix.at[s], lambda s: landed.at[s], device_of, send_b, recv_b)()
    landed[me] = prefix[me]
    out_ref[...] = landed[...]


def step_kernel(
    n_seq, n_opt, part_ref, w_ref, code_ref, scale_ref, row_ref, col_ref,
    update_ref, code_out, scale_out, row_out, col_out,
    got_a, mid, got_b, stats, all_stats, peak, all_peaks,
    send_a, recv_a, send_b, recv_b, send_c, recv_c, send_d, recv_d,
):
    seq = lax.axis_index("seq")
    opt = lax.axis_index("opt")
    n = n_seq * n_opt
    me = seq * n_opt + opt

    def any_device(i):
        return (i // n_opt, lax.rem(i, n_opt))

    greet(n, me, any_device)
    begin_swap(
        n_opt, opt, lambda o: part_ref.at[o], lambda o: got_a.at[o],
        lambda o: (seq, o), send_a, recv_a,
    )()
    got_a[opt] = part_ref[opt]

    def fold(s, carry):
        total = got_a[0, s].astype(f32)
        for o in range(1, n_opt):
            total += got_a[o, s].astype(f32)
        mid[s] = total.astype(bf16)
        return carry

    lax.fori_loop(0, n_seq, fold, 0)
    begin_swap(
        n_seq, seq, lambda s: mid.at[s], lambda s: got_b.at[s],
        lambda s: (s, opt), send_b, recv_b,
    )()
    got_b[seq] = mid[seq]
    grad = got_b[0].astype(f32)
    for s in range(1, n_seq):
        grad += got_b[s].astype(f32)

    rows, cols = grad.shape
    width = n * rows
    squares_raw = grad * grad
    stats[:, :cols] = jnp.sum(squares_raw, axis=0, keepdims=True)
    row_stat = row_ref[...]
    stats[:, cols:] = jnp.broadcast_to(jnp.sum(row_stat, axis=0, keepdims=True), (1, LANES))
    begin_swap(
        n, me, lambda i: stats, lambda i: all_stats.at[i], any_device, send_c, recv_c
    )()
    all_stats[me] = stats[...]
    sums = all_stats[0]
    for i in range(1, n):
        sums += all_stats[i]
    col_raw = sums[:, :cols]
    old_total = sums[:, cols : cols + 1]
    raw_total = jnp.sum(col_raw, axis=1, keepdims=True)
    factor = jnp.minimum(1.0, clip_norm / jnp.sqrt(raw_total + norm_floor))
    scaled = grad * factor
    moment = beta_one * code_ref[...].astype(f32) * scale_ref[...] + (1.0 - beta_one) * scaled
    peak[...] = jnp.max(jnp.abs(moment), axis=0, keepdims=True)
    end_peaks = begin_swap(
        n, me, lambda i: peak, lambda i: all_peaks.at[i], any_device, send_d, recv_d
    )
    col_next = beta_two * col_ref[...] + (1.0 - beta_two) * (
        factor * factor * col_raw / width + tiny_square
    )
    row_next = beta_two * row_stat + (1.0 - beta_two) * (
        jnp.sum(scaled * scaled, axis=1, keepdims=True) / cols + tiny_square
    )
    row_mean = (
        beta_two * old_total
        + (1.0 - beta_two) * (factor * factor * raw_total / cols + width * tiny_square)
    ) / width
    second = row_next * col_next / row_mean
    update_ref[...] = moment / (jnp.sqrt(second) + adam_floor) + weight_decay * w_ref[...]
    row_out[...] = row_next
    col_out[...] = col_next
    end_peaks()
    all_peaks[me] = peak[...]
    scale_next = all_peaks[0]
    for i in range(1, n):
        scale_next = jnp.maximum(scale_next, all_peaks[i])
    scale_next = scale_next + peak_floor
    scale_out[...] = scale_next
    code_out[...] = (moment / scale_next).astype(bf16)


def params(**more):
    return pltpu.CompilerParams(vmem_limit_bytes=VMEM_LIMIT, **more)


def whole():
    return pl.BlockSpec(memory_space=pltpu.VMEM)


def dma(*counts):
    return [pltpu.SemaphoreType.DMA((count,)) for count in counts for _ in range(2)]


def per_device(
    n_seq, n_opt, layer_in, ssm_input, grad_out, log_decay, skip_gain, w_bc, m_code, m_scale,
    row_stat, col_stat,
):
    layer_rows = layer_in[0]
    x = ssm_input[0]
    dy = grad_out[0]
    length, width = layer_rows.shape
    heads = skip_gain.shape[0]
    head_dim = x.shape[1] // heads
    state_dim = w_bc.shape[1] // 2
    count = length // BLOCK
    group = heads // n_seq
    own_rows = w_bc.shape[0]

    ones = (
        lax.broadcasted_iota(jnp.int32, (BLOCK, BLOCK), 0)
        <= lax.broadcasted_iota(jnp.int32, (BLOCK, BLOCK), 1)
    ).astype(f32)
    running = jnp.dot(
        log_decay[0].reshape(heads * count, BLOCK), ones, precision=highest
    ).reshape(heads, count, BLOCK)
    decay = jnp.exp(jnp.sum(running[:, :, BLOCK - 1], axis=1))
    decay = jnp.broadcast_to(decay[:, None], (heads, LANES)).reshape(n_seq, group, 1, LANES)

    tokens = pl.BlockSpec((length, head_dim), lambda h: (0, h))
    run_spec = pl.BlockSpec((1, count, BLOCK), lambda h: (h, 0, 0))
    mix_spec = pl.BlockSpec((count, BLOCK, BLOCK), lambda h: (0, 0, 0))
    state_spec = pl.BlockSpec((1, count, state_dim, head_dim), lambda h: (h, 0, 0, 0))
    far_spec = pl.BlockSpec(
        (1, 2, 1, state_dim, head_dim), lambda h: (h // group, 0, h % group, 0, 0)
    )
    b_spec = pl.BlockSpec((length, state_dim), lambda h: (0, 0))
    c_spec = pl.BlockSpec((length, state_dim), lambda h: (0, 1))
    far_shape = (n_seq, 2, group, state_dim, head_dim)

    w_shape = (own_rows, 2 * state_dim)
    mixing, w_all = pl.pallas_call(
        functools.partial(mixing_kernel, count, n_seq, n_opt),
        grid=(heads,),
        in_specs=[whole(), tokens, tokens, run_spec],
        out_specs=[mix_spec, whole()],
        out_shape=[
            jax.ShapeDtypeStruct((count, BLOCK, BLOCK), f32),
            jax.ShapeDtypeStruct((n_seq, n_opt) + w_shape, bf16),
        ],
        scratch_shapes=[pltpu.VMEM((n_opt, n_seq) + w_shape, bf16)] + dma(n_seq, n_opt),
        compiler_params=params(collective_id=2, has_side_effects=True),
        name="gather_and_mixing",
    )(w_bc.astype(bf16), x, dy, running)
    w_all = w_all.reshape(width, 2 * state_dim)

    proj = jnp.dot(layer_rows, w_all, preferred_element_type=f32).astype(bf16)

    sent, starts, outs = pl.pallas_call(
        functools.partial(local_kernel, count),
        grid=(heads,),
        in_specs=[tokens, tokens, b_spec, c_spec, run_spec],
        out_specs=[far_spec, state_spec, state_spec],
        out_shape=[
            jax.ShapeDtypeStruct(far_shape, bf16),
            jax.ShapeDtypeStruct((heads, count, state_dim, head_dim), bf16),
            jax.ShapeDtypeStruct((heads, count, state_dim, head_dim), bf16),
        ],
        scratch_shapes=[pltpu.VMEM((state_dim, length), f32)] * 2,
        compiler_params=params(),
        name="local_states",
    )(x, dy, proj, proj, running)

    far = pl.pallas_call(
        functools.partial(carry_kernel, n_seq),
        in_specs=[whole(), whole()],
        out_specs=whole(),
        out_shape=jax.ShapeDtypeStruct(far_shape, bf16),
        scratch_shapes=[
            pltpu.VMEM(far_shape, bf16),
            pltpu.VMEM((n_seq, group, 1, LANES), f32),
            pltpu.VMEM(far_shape, bf16),
            pltpu.VMEM(far_shape, bf16),
            pltpu.VMEM(far_shape[1:], f32),
        ]
        + dma(n_seq, n_seq, n_seq),
        compiler_params=params(collective_id=0, has_side_effects=True),
        name="carry_states",
    )(sent, decay)

    grad_input, grad_bc = pl.pallas_call(
        functools.partial(grads_kernel, count),
        grid=(heads,),
        in_specs=[
            pl.BlockSpec(memory_space=pltpu.SMEM), tokens, tokens, b_spec, c_spec, run_spec,
            state_spec, state_spec, far_spec, mix_spec,
        ],
        out_specs=[tokens, pl.BlockSpec((length, 2 * state_dim), lambda h: (0, 0))],
        out_shape=[
            jax.ShapeDtypeStruct(x.shape, bf16),
            jax.ShapeDtypeStruct((length, 2 * state_dim), bf16),
        ],
        scratch_shapes=[
            pltpu.VMEM((count, BLOCK, BLOCK), f32),
            pltpu.VMEM((length, state_dim), f32),
            pltpu.VMEM((length, state_dim), f32),
        ],
        compiler_params=params(),
        name="grads",
    )(skip_gain, x, dy, proj, proj, running, starts, outs, far, mixing)

    cols = 2 * state_dim
    part = lax.dot_general(
        layer_rows, grad_bc, (((0,), (0,)), ((), ())), preferred_element_type=f32
    ).astype(bf16)
    part = jnp.transpose(part.reshape(n_seq, n_opt, own_rows, cols), (1, 0, 2, 3))

    n = n_seq * n_opt
    update, code_next, scale_next, row_next, col_next = pl.pallas_call(
        functools.partial(step_kernel, n_seq, n_opt),
        in_specs=[whole()] * 6,
        out_specs=[whole()] * 5,
        out_shape=[
            jax.ShapeDtypeStruct((own_rows, cols), f32),
            jax.ShapeDtypeStruct((own_rows, cols), bf16),
            jax.ShapeDtypeStruct((1, cols), f32),
            jax.ShapeDtypeStruct((own_rows, 1), f32),
            jax.ShapeDtypeStruct((1, cols), f32),
        ],
        scratch_shapes=[
            pltpu.VMEM((n_opt, n_seq, own_rows, cols), bf16),
            pltpu.VMEM((n_seq, own_rows, cols), bf16),
            pltpu.VMEM((n_seq, own_rows, cols), bf16),
            pltpu.VMEM((1, cols + LANES), f32),
            pltpu.VMEM((n, 1, cols + LANES), f32),
            pltpu.VMEM((1, cols), f32),
            pltpu.VMEM((n, 1, cols), f32),
        ]
        + dma(n_opt, n_seq, n, n),
        compiler_params=params(collective_id=1, has_side_effects=True),
        name="sum_and_step",
    )(part, w_bc, m_code, m_scale[None, :], row_stat[:, None], col_stat[None, :])
    return (grad_input[None], update, code_next, scale_next[0], row_next[:, 0], col_next[0])


def solution(mesh):
    return jax.shard_map(
        functools.partial(per_device, mesh.shape["seq"], mesh.shape["opt"]),
        mesh=mesh,
        in_specs=(
            P("opt", "seq", None),
            P("opt", "seq", None),
            P("opt", "seq", None),
            P("opt", None, "seq"),
            P(),
            P(("seq", "opt"), None),
            P(("seq", "opt"), None),
            P(),
            P(("seq", "opt")),
            P(),
        ),
        out_specs=(
            P("opt", "seq", None),
            P(("seq", "opt"), None),
            P(("seq", "opt"), None),
            P(),
            P(("seq", "opt")),
            P(),
        ),
        check_vma=False,
    )
```
